32 devices in a mesh: gx: 4 (over x, core), gy: 8 (over z, y).
Axes of the slice: x: 2, y: 2, z: 4, core: 2. Of those that a mesh axis runs over, the one named last changes fastest.
Arguments:
- krylov_basis: float32 [144, 32, 64, 256], P(None, 'gx', 'gy'), may hold values from -6 to 6
- advection: float32 [3, 32, 64, 256], P(None, 'gx', 'gy'), may hold values from -0.6 to 0.6
- reaction: float32 [32, 64, 256], P('gx', 'gy'), may hold values from 0.1 to 2
Outputs:
- block_one: float32 [16, 32, 64, 256], P(None, 'gx', 'gy')
- block_two: float32 [16, 32, 64, 256], P(None, 'gx', 'gy')
- coeff_one: float32 [144, 16], replicated
- coeff_two: float32 [160, 16], replicated
- upper_one: float32 [16, 16], replicated
- upper_two: float32 [16, 16], replicated
The draws below stay inside these ranges and needn't reach their ends.
All inputs are finite; a program needn't handle non-finite values.
Results may differ from the reference program's by a relative error of at most 0.0003.
Values sent between devices are 32-bit elements; how exact they have to be, the bound alone decides.
A program may use at most 128 MiB of HBM per device.

```python
import math
import jax
import jax.numpy as jnp
from jax import lax

BLOCK = 16
PRIOR = 9
NZ = 256
NX = 32
NY = 64


def draw_krylov_basis(key, part):
    row_count = PRIOR * BLOCK
    noise_key = jax.random.fold_in(key, 11)
    partner_key = jax.random.fold_in(key, 23)
    partner = jax.random.permutation(partner_key, row_count)
    fields = jax.random.normal(noise_key, (row_count, NX, NY, NZ), jnp.float32)
    mixing = 0.3
    blended = (fields + mixing * fields[partner]) / jnp.sqrt(1.0 + mixing * mixing)
    return jnp.clip(blended, -6.0, 6.0).astype(jnp.float32)


def levels(own_key, dims, pieces, low, top_value):
    gain = 1.0
    for position, shards_of in pieces:
        steps = jax.random.uniform(jax.random.fold_in(jax.random.fold_in(own_key, 6), position), (shards_of,), jnp.float32, low / len(pieces), top_value / len(pieces))
        gain = gain * jnp.repeat(jnp.exp(steps), dims[position] // shards_of).reshape((-1,) + (1,) * (len(dims) - 1 - position))
    return gain


def setup_inputs(seed: int = 0) -> dict:
    key_of = jax.random.split(jax.random.key(seed), 4)
    return {
        "krylov_basis": draw_krylov_basis(jax.random.fold_in(key_of[3], 71), 0),
        "advection": jnp.clip(jax.random.uniform(key_of[1], (3, NX, NY, NZ), jnp.float32, -0.6, 0.6) * levels(key_of[1], (3, NX, NY, NZ), ((1, 4), (2, 8)), -0.4, 0.0), -0.6, 0.6),
        "reaction": jnp.clip(jnp.exp(math.log(2.0) - 2.9957323 * jax.random.uniform(key_of[2], (NX, NY, NZ), jnp.float32) ** levels(key_of[2], (NX, NY, NZ), ((0, 4), (1, 8)), -0.2, 0.2)), 0.1, 2.0),
    }


HIGHEST = lax.Precision.HIGHEST

def inner_cells(left, right):
    return lax.dot_general(left.astype(jnp.float32), right.astype(jnp.float32), (((1,), (1,)), ((), ())), precision=HIGHEST, preferred_element_type=jnp.float32)

def project(coeffs, bases):
    offset = 0
    summed = None
    for base in bases:
        height = base.shape[0]
        update = jnp.dot(coeffs[offset:offset + height].T, base, precision=HIGHEST)
        summed = update if summed is None else summed + update
        offset = offset + height
    return summed

def apply_operator(values, advection, reaction):
    padded = jnp.pad(values, ((0, 0), (1, 1), (1, 1), (1, 1)))
    neighbours = (1.0 + advection[0]) * padded[:, :-2, 1:-1, 1:-1] + (1.0 - advection[0]) * padded[:, 2:, 1:-1, 1:-1]
    neighbours = neighbours + (1.0 + advection[1]) * padded[:, 1:-1, :-2, 1:-1] + (1.0 - advection[1]) * padded[:, 1:-1, 2:, 1:-1]
    neighbours = neighbours + (1.0 + advection[2]) * padded[:, 1:-1, 1:-1, :-2] + (1.0 - advection[2]) * padded[:, 1:-1, 1:-1, 2:]
    return (6.0 + reaction) * values - neighbours

def orthonormalize(values, bases, cell_total):
    first_coef = jnp.concatenate([inner_cells(base, values) for base in bases], 0) / cell_total
    values = values - project(first_coef, bases)
    second = jnp.concatenate([inner_cells(base, values) for base in bases], 0) / cell_total
    values = values - project(second, bases)
    gram_matrix = inner_cells(values, values) / cell_total
    lower_factor = jnp.linalg.cholesky(gram_matrix)
    inverse = jax.scipy.linalg.solve_triangular(lower_factor, jnp.eye(values.shape[0], dtype=jnp.float32), lower=True)
    new_block = jnp.dot(inverse, values, precision=HIGHEST)
    return (new_block, first_coef + second, lower_factor.T)

def reference(krylov_basis, advection, reaction):
    row_count = krylov_basis.shape[0]
    grid_shape = krylov_basis.shape[1:]
    cell_total = float(grid_shape[0] * grid_shape[1] * grid_shape[2])
    basis_flat = krylov_basis.reshape(row_count, -1)
    latest = krylov_basis[row_count - BLOCK:]
    image = apply_operator(latest, advection, reaction).reshape(BLOCK, -1)
    block_one, coeff_one, upper_one = orthonormalize(image, (basis_flat,), cell_total)
    image = apply_operator(block_one.reshape((BLOCK,) + grid_shape), advection, reaction).reshape(BLOCK, -1)
    block_two, coeff_two, upper_two = orthonormalize(image, (basis_flat, block_one), cell_total)
    return (block_one.reshape((BLOCK,) + grid_shape), block_two.reshape((BLOCK,) + grid_shape), coeff_one, coeff_two, upper_one, upper_two)
```

```python
import functools

import jax
import jax.numpy as jnp
from jax import lax
from jax.experimental import pallas as pl
from jax.experimental.pallas import tpu as pltpu
from jax.sharding import PartitionSpec as P

BLOCK = 16
LANES = 128
WIDE = 256
MESH = pl.DeviceIdType.MESH
HIGHEST = lax.Precision.HIGHEST
F32 = jnp.float32
BF16 = jnp.bfloat16


def exact(left, right, nt=False):
    dims = (((1,), (1 if nt else 0,)), ((), ()))
    return lax.dot_general(left, right, dims, precision=HIGHEST, preferred_element_type=F32)


def quick(left, right, nt=False):
    dims = (((1,), (1 if nt else 0,)), ((), ()))
    return lax.dot_general(left, right, dims, preferred_element_type=F32)


def split(values):
    high = values.astype(BF16)
    low = (values - high.astype(F32)).astype(BF16)
    return high, low


def sum_everywhere(nx, ny, own, first, part, second, done, whole, sems):
    gx, gy = lax.axis_index("gx"), lax.axis_index("gy")
    height = part.shape[0]
    send1, recv1, send2, recv2, send3, recv3 = sems
    mine = pl.ds(pl.multiple_of(gx * height, 8), height)
    copies = []
    for d in range(1, nx):
        peer = lax.rem(gx + d, nx)
        copies.append(
            pltpu.make_async_remote_copy(
                src_ref=own.at[pl.ds(pl.multiple_of(peer * height, 8), height)],
                dst_ref=first.at[d - 1],
                send_sem=send1.at[d - 1],
                recv_sem=recv1.at[d - 1],
                device_id=(peer, gy),
                device_id_type=MESH,
            )
        )
    for copy in copies:
        copy.start()
    for copy in copies:
        copy.wait_recv()
    total = own[mine, :]
    for d in range(1, nx):
        total = total + first[d - 1]
    part[...] = total
    second[gy] = total
    across = []
    for d in range(1, ny):
        peer = lax.rem(gy + d, ny)
        across.append(
            pltpu.make_async_remote_copy(
                src_ref=part,
                dst_ref=second.at[gy],
                send_sem=send2.at[d - 1],
                recv_sem=recv2.at[d - 1],
                device_id=(gx, peer),
                device_id_type=MESH,
            )
        )
    for copy in across:
        copy.start()
    for copy in across:
        copy.wait_recv()
    total = second[0]
    for s in range(1, ny):
        total = total + second[s]
    done[...] = total
    whole[mine, :] = total
    back = []
    for d in range(1, nx):
        peer = lax.rem(gx + d, nx)
        back.append(
            pltpu.make_async_remote_copy(
                src_ref=done,
                dst_ref=whole.at[mine],
                send_sem=send3.at[d - 1],
                recv_sem=recv3.at[d - 1],
                device_id=(peer, gy),
                device_id_type=MESH,
            )
        )
    for copy in back:
        copy.start()
    for copy in back:
        copy.wait_recv()
    for copy in copies + across + back:
        copy.wait_send()


def factor(gram):
    n = gram.shape[0]
    row = lax.broadcasted_iota(jnp.int32, (n, n), 0)
    col = lax.broadcasted_iota(jnp.int32, (n, n), 1)
    both = jnp.concatenate([gram, (row == col).astype(F32)], axis=1)
    wide_row = lax.broadcasted_iota(jnp.int32, (n, 2 * n), 0)
    for k in range(n):
        scale = 1.0 / jnp.sqrt(both[k : k + 1, k : k + 1])
        pivot = both[k : k + 1, :] * scale
        column = both[:, k : k + 1] * scale
        both = jnp.where(
            wide_row > k, both - column * pivot, jnp.where(wide_row == k, pivot, both)
        )
    return jnp.where(col >= row, both[:, :n], 0.0), both[:, n:]


def solve_small(count, sums, metric, cells):
    col = lax.broadcasted_iota(jnp.int32, (BLOCK, WIDE), 1)
    row = lax.broadcasted_iota(jnp.int32, (BLOCK, WIDE), 0)
    sums = sums * (1.0 / cells)
    first = jnp.where(col < count, sums, 0.0)
    square = sums[:, count : count + BLOCK]
    coeff = 2.0 * first - exact(first, metric)
    seen = exact(coeff, metric)
    gram = square - 2.0 * exact(coeff, first, nt=True) + exact(seen, coeff, nt=True)
    upper, inverse = factor(gram)
    pick = jnp.where(col == row + count, 1.0, 0.0)
    combine = exact(inverse, pick - coeff)
    left = exact(inverse, first - seen)
    return coeff, upper, combine, left


def kernel(
    nx, ny,
    v_hbm, adv, rea,
    one_hbm, two_hbm, coeff1, coeff2, upper1, upper2,
    vf, bh, bl, uf, qf, pf, acc, hacc, metric,
    own1, first1, part1, second1, done1, whole1,
    own2, first2, part2, second2, done2, whole2,
    vsem, usem, osem1, osem2, hs1, hr1, hs2, hr2,
    *sems,
):
    rows, X, Y, Z = v_hbm.shape
    main = rows - BLOCK
    cells = float(X * Y * Z * nx * ny)
    gx, gy = lax.axis_index("gx"), lax.axis_index("gy")

    def load_u(p):
        x, y = p // Y, p % Y
        return pltpu.make_async_copy(
            v_hbm.at[pl.ds(main, BLOCK), x, y], uf.at[x + 1, y + 1], usem.at[p]
        )

    def load_v(p):
        x, y = p // Y, p % Y
        return pltpu.make_async_copy(v_hbm.at[pl.ds(0, main), x, y], vf.at[p], vsem.at[p])

    def loop(n, f):
        lax.fori_loop(0, n, lambda i, c: (f(i), c)[1], 0)

    loop(X * Y, lambda p: load_u(p).start())
    loop(X * Y, lambda p: load_v(p).start())

    barrier = pltpu.get_barrier_semaphore()
    for d in range(1, nx):
        pl.semaphore_signal(
            barrier, inc=1, device_id=(lax.rem(gx + d, nx), gy), device_id_type=MESH
        )
    for d in range(1, ny):
        pl.semaphore_signal(
            barrier, inc=1, device_id=(gx, lax.rem(gy + d, ny)), device_id_type=MESH
        )

    acc[...] = jnp.zeros_like(acc)
    hacc[...] = jnp.zeros_like(hacc)
    metric[...] = jnp.zeros_like(metric)
    own1[...] = jnp.zeros_like(own1)
    own2[...] = jnp.zeros_like(own2)
    edge_x = jnp.zeros((1, Y, BLOCK, Z), F32)
    edge_y = jnp.zeros((X, 1, BLOCK, Z), F32)
    for field in (uf, qf):

        @pl.when(gx == 0)
        def _(field=field):
            field[0:1, 1 : Y + 1] = edge_x

        @pl.when(gx == nx - 1)
        def _(field=field):
            field[X + 1 : X + 2, 1 : Y + 1] = edge_x

        @pl.when(gy == 0)
        def _(field=field):
            field[1 : X + 1, 0:1] = edge_y

        @pl.when(gy == ny - 1)
        def _(field=field):
            field[1 : X + 1, Y + 1 : Y + 2] = edge_y

    def borders(field, ss, rs):
        xs, ys = pl.ds(1, X), pl.ds(1, Y)
        up, down = lax.rem(gx + 1, nx), lax.rem(gx + nx - 1, nx)
        right, left = lax.rem(gy + 1, ny), lax.rem(gy + ny - 1, ny)

        def make(i, src, dst, dev):
            return pltpu.make_async_remote_copy(
                src_ref=src, dst_ref=dst, send_sem=ss.at[i], recv_sem=rs.at[i],
                device_id=dev, device_id_type=MESH,
            )

        return (
            (gx < nx - 1, gx > 0, make(0, field.at[X, ys], field.at[0, ys], (up, gy))),
            (gx > 0, gx < nx - 1, make(1, field.at[1, ys], field.at[X + 1, ys], (down, gy))),
            (gy < ny - 1, gy > 0, make(2, field.at[xs, Y], field.at[xs, 0], (gx, right))),
            (gy > 0, gy < ny - 1, make(3, field.at[xs, 1], field.at[xs, Y + 1], (gx, left))),
        )

    def send(parts):
        for sends, gets, copy in parts:
            pl.when(sends)(copy.start)

    def receive(parts):
        for sends, gets, copy in parts:
            pl.when(gets)(copy.wait_recv)

    def sent(parts):
        for sends, gets, copy in parts:
            pl.when(sends)(copy.wait_send)

    loop(X * Y, lambda p: load_u(p).wait())
    pl.semaphore_wait(barrier, nx - 1 + ny - 1)
    border1 = borders(uf, hs1, hr1)
    send(border1)

    def gram(p):
        load_v(p).wait()
        vh, vl = split(vf[p])
        uh, ul = split(uf[p // Y + 1, p % Y + 1])
        high = jnp.concatenate([vh, uh], 0)
        low = jnp.concatenate([vl, ul], 0)
        bh[p, 0:rows, :] = high
        bl[p, 0:rows, :] = low
        r = quick(jnp.concatenate([high, low], 0), high, nt=True)
        acc[0:rows, 0:rows] += r[:rows]
        acc[WIDE : WIDE + rows, 0:rows] += r[rows:]

    loop(X * Y, gram)

    lane = lax.broadcasted_iota(jnp.int32, (BLOCK, Z), 1)

    def image(field, height):
        def step(x):
            total = jnp.zeros((height + BLOCK, 2 * BLOCK), F32)
            for y in range(Y):
                here = field[x + 1, y + 1]
                a0 = adv[0, x, y : y + 1, :]
                a1 = adv[1, x, y : y + 1, :]
                a2 = adv[2, x, y : y + 1, :]
                below = jnp.where(lane == 0, 0.0, pltpu.roll(here, 1, 1))
                above = jnp.where(lane == Z - 1, 0.0, pltpu.roll(here, Z - 1, 1))
                near = (1.0 + a0) * field[x, y + 1] + (1.0 - a0) * field[x + 2, y + 1]
                near = near + (1.0 + a1) * field[x + 1, y] + (1.0 - a1) * field[x + 1, y + 2]
                near = near + (1.0 + a2) * below + (1.0 - a2) * above
                w = (6.0 + rea[x, y : y + 1, :]) * here - near
                p = x * Y + y
                wh, wl = split(w)
                bh[p, height : height + BLOCK, :] = wh
                bl[p, height : height + BLOCK, :] = wl
                both = jnp.concatenate([wh, wl], 0)
                total = total + quick(jnp.concatenate([bh[p, 0:height, :], wh], 0), both, nt=True)
                total = total + quick(jnp.concatenate([bl[p, 0:height, :], wl], 0), both, nt=True)
            hacc[0 : height + BLOCK, 0 : 2 * BLOCK] += total

        loop(X, step)
        turned = hacc[...].T
        return turned[0:BLOCK] + turned[BLOCK : 2 * BLOCK]

    receive(border1)
    dots = image(uf, rows)
    cross = acc[WIDE : 2 * WIDE, :]
    local = acc[0:WIDE, :] + cross + cross.T
    own1[0:main, :] = local[0:main, 0:main]
    own1[main : main + 16, :] = local[main : main + 16, 0:main]
    own1[main + 16 : main + 32, :] = local[main : main + 16, main:WIDE]
    own1[main + 32 : main + 48, :] = dots[:, 0:main]
    own1[main + 48 : main + 64, :] = dots[:, main:WIDE]
    sum_everywhere(nx, ny, own1, first1, part1, second1, done1, whole1, sems[0:6])

    metric[0:main, 0:main] = whole1[0:main, :] * (1.0 / cells)
    metric[main : main + 16, 0:main] = whole1[main : main + 16, :] * (1.0 / cells)
    metric[main : main + 16, main:WIDE] = whole1[main + 16 : main + 32, :] * (1.0 / cells)
    metric[0:main, main:WIDE] = metric[main:WIDE, 0:main].T
    sums = jnp.concatenate([whole1[main + 32 : main + 48, :], whole1[main + 48 : main + 64, :]], 1)
    coeff, upper, combine, left = solve_small(rows, sums, metric[...], cells)
    coeff1[...] = coeff
    upper1[...] = upper

    def assemble(combine, height, put):
        ch, cl = split(combine)
        both = jnp.concatenate([ch, cl], 0)[:, 0:height]

        def step(x):
            for y in range(Y):
                p = x * Y + y
                r = quick(both, bh[p, 0:height, :]) + quick(both, bl[p, 0:height, :])
                put(x, y, p, r[0:BLOCK] + r[BLOCK : 2 * BLOCK])

        loop(X, step)

    def put_one(x, y, p, q):
        qf[x + 1, y + 1] = q
        qh, ql = split(q)
        bh[p, rows : rows + BLOCK, :] = qh
        bl[p, rows : rows + BLOCK, :] = ql

    assemble(combine, rows + BLOCK, put_one)
    border2 = borders(qf, hs2, hr2)
    send(border2)

    def store_one(p):
        x, y = p // Y, p % Y
        return pltpu.make_async_copy(qf.at[x + 1, y + 1], one_hbm.at[:, x, y], osem1.at[p])

    loop(X * Y, lambda p: store_one(p).start())

    extra = jnp.concatenate(
        [jnp.zeros((16, WIDE), F32), left, jnp.zeros((LANES - 32, WIDE), F32)], 0
    )
    metric[main:WIDE, :] += extra
    metric[0:main, main:WIDE] += extra[:, 0:main].T
    r = lax.broadcasted_iota(jnp.int32, (LANES, LANES), 0)
    c = lax.broadcasted_iota(jnp.int32, (LANES, LANES), 1)
    unit = jnp.where((r == c) & (r >= 16) & (r < 32), 1.0, 0.0)
    metric[main:WIDE, main:WIDE] += extra[:, main:WIDE].T + unit

    hacc[...] = jnp.zeros_like(hacc)
    receive(border2)
    dots = image(qf, rows + BLOCK)
    own2[0:16, :] = dots[:, 0:main]
    own2[16:32, :] = dots[:, main:WIDE]
    sum_everywhere(nx, ny, own2, first2, part2, second2, done2, whole2, sems[6:12])
    sums = jnp.concatenate([whole2[0:16, :], whole2[16:32, :]], 1)
    coeff, upper, combine, left = solve_small(rows + BLOCK, sums, metric[...], cells)
    coeff2[...] = coeff
    upper2[...] = upper

    def put_two(x, y, p, q):
        pf[x, y] = q

    assemble(combine, rows + 2 * BLOCK, put_two)

    def store_two(p):
        x, y = p // Y, p % Y
        return pltpu.make_async_copy(pf.at[x, y], two_hbm.at[:, x, y], osem2.at[p])

    loop(X * Y, lambda p: store_two(p).start())
    sent(border1)
    sent(border2)
    loop(X * Y, lambda p: store_one(p).wait())
    loop(X * Y, lambda p: store_two(p).wait())


def body(nx, ny, krylov_basis, advection, reaction):
    rows, X, Y, Z = krylov_basis.shape
    height1 = rows - BLOCK + 64
    height2 = max(32, 8 * nx)
    dma = pltpu.SemaphoreType.DMA
    field = jax.ShapeDtypeStruct((BLOCK, X, Y, Z), F32)
    sum_scratch = []
    for height in (height1, height2):
        sum_scratch += [
            pltpu.VMEM((height, LANES), F32),
            pltpu.VMEM((nx - 1, height // nx, LANES), F32),
            pltpu.VMEM((height // nx, LANES), F32),
            pltpu.VMEM((ny, height // nx, LANES), F32),
            pltpu.VMEM((height // nx, LANES), F32),
            pltpu.VMEM((height, LANES), F32),
        ]
    sum_sems = [dma((n - 1,)) for n in (nx, nx, ny, ny, nx, nx)] * 2
    vmem = pl.BlockSpec(memory_space=pltpu.VMEM)
    hbm = pl.BlockSpec(memory_space=pl.ANY)
    one, two, coeff1, coeff2, upper1, upper2 = pl.pallas_call(
        functools.partial(kernel, nx, ny),
        out_shape=(
            field,
            field,
            jax.ShapeDtypeStruct((BLOCK, WIDE), F32),
            jax.ShapeDtypeStruct((BLOCK, WIDE), F32),
            jax.ShapeDtypeStruct((BLOCK, BLOCK), F32),
            jax.ShapeDtypeStruct((BLOCK, BLOCK), F32),
        ),
        in_specs=[hbm, vmem, vmem],
        out_specs=(hbm, hbm, vmem, vmem, vmem, vmem),
        scratch_shapes=[
            pltpu.VMEM((X * Y, rows - BLOCK, Z), F32),
            pltpu.VMEM((X * Y, rows + 2 * BLOCK, Z), BF16),
            pltpu.VMEM((X * Y, rows + 2 * BLOCK, Z), BF16),
            pltpu.VMEM((X + 2, Y + 2, BLOCK, Z), F32),
            pltpu.VMEM((X + 2, Y + 2, BLOCK, Z), F32),
            pltpu.VMEM((X, Y, BLOCK, Z), F32),
            pltpu.VMEM((2 * WIDE, WIDE), F32),
            pltpu.VMEM((WIDE, LANES), F32),
            pltpu.VMEM((WIDE, WIDE), F32),
        ]
        + sum_scratch
        + [dma((X * Y,))] * 4
        + [dma((4,))] * 4
        + sum_sems,
        compiler_params=pltpu.CompilerParams(
            collective_id=0, has_side_effects=True, vmem_limit_bytes=56 * 1024 * 1024
        ),
    )(krylov_basis, advection, reaction)
    return (one, two, coeff1[:, :rows].T, coeff2[:, : rows + BLOCK].T, upper1, upper2)


def solution(mesh):
    return jax.shard_map(
        functools.partial(body, mesh.shape["gx"], mesh.shape["gy"]),
        mesh=mesh,
        in_specs=(P(None, "gx", "gy", None), P(None, "gx", "gy", None), P("gx", "gy", None)),
        out_specs=(P(None, "gx", "gy", None), P(None, "gx", "gy", None), P(), P(), P(), P()),
        check_vma=False,
    )
```

```python
import functools

import jax
import jax.numpy as jnp
from jax import lax
from jax.experimental import pallas as pl
from jax.experimental.pallas import tpu as pltpu
from jax.sharding import PartitionSpec as P

BLOCK = 16
LANES = 128
WIDE = 256
MESH = pl.DeviceIdType.MESH
HIGHEST = lax.Precision.HIGHEST
F32 = jnp.float32
BF16 = jnp.bfloat16


def exact(left, right, nt=False):
    dims = (((1,), (1 if nt else 0,)), ((), ()))
    return lax.dot_general(left, right, dims, precision=HIGHEST, preferred_element_type=F32)


def quick(left, right, nt=False):
    dims = (((1,), (1 if nt else 0,)), ((), ()))
    return lax.dot_general(left, right, dims, preferred_element_type=F32)


def split(values):
    high = values.astype(BF16)
    low = (values - high.astype(F32)).astype(BF16)
    return high, low


def loop(n, f):
    lax.fori_loop(0, n, lambda i, c: (f(i), c)[1], 0)


def over_edges(X, Y, step):
    loop(2, lambda i: step(i * (X - 1), range(Y)))
    loop(X - 2, lambda i: step(i + 1, (0, Y - 1)))


def over_inside(X, Y, step):
    loop(X - 2, lambda i: step(i + 1, range(1, Y - 1)))


def assemble(bh, bl, X, Y, combine, height, put):
    ch, cl = split(combine)
    both = jnp.concatenate([ch, cl], 0)[:, 0:height]

    def step(x, ys):
        for y in ys:
            p = x * Y + y
            r = quick(both, bh[p, 0:height, :]) + quick(both, bl[p, 0:height, :])
            put(x, y, p, r[0:BLOCK] + r[BLOCK : 2 * BLOCK])

    return step


def sum_everywhere(nx, ny, own, first, part, second, done, whole, sems):
    gx, gy = lax.axis_index("gx"), lax.axis_index("gy")
    height = part.shape[0]
    send1, recv1, send2, recv2, send3, recv3 = sems
    mine = pl.ds(pl.multiple_of(gx * height, 8), height)
    copies = []
    for d in range(1, nx):
        peer = lax.rem(gx + d, nx)
        copies.append(
            pltpu.make_async_remote_copy(
                src_ref=own.at[pl.ds(pl.multiple_of(peer * height, 8), height)],
                dst_ref=first.at[d - 1],
                send_sem=send1.at[d - 1],
                recv_sem=recv1.at[d - 1],
                device_id=(peer, gy),
                device_id_type=MESH,
            )
        )
    for copy in copies:
        copy.start()
    for copy in copies:
        copy.wait_recv()
    total = own[mine, :]
    for d in range(1, nx):
        total = total + first[d - 1]
    part[...] = total
    second[gy] = total
    across = []
    for d in range(1, ny):
        peer = lax.rem(gy + d, ny)
        across.append(
            pltpu.make_async_remote_copy(
                src_ref=part,
                dst_ref=second.at[gy],
                send_sem=send2.at[d - 1],
                recv_sem=recv2.at[d - 1],
                device_id=(gx, peer),
                device_id_type=MESH,
            )
        )
    for copy in across:
        copy.start()
    for copy in across:
        copy.wait_recv()
    total = second[0]
    for s in range(1, ny):
        total = total + second[s]
    done[...] = total
    whole[mine, :] = total
    back = []
    for d in range(1, nx):
        peer = lax.rem(gx + d, nx)
        back.append(
            pltpu.make_async_remote_copy(
                src_ref=done,
                dst_ref=whole.at[mine],
                send_sem=send3.at[d - 1],
                recv_sem=recv3.at[d - 1],
                device_id=(peer, gy),
                device_id_type=MESH,
            )
        )
    for copy in back:
        copy.start()
    for copy in back:
        copy.wait_recv()
    for copy in copies + across + back:
        copy.wait_send()


def factor(gram):
    n = gram.shape[0]
    row = lax.broadcasted_iota(jnp.int32, (n, n), 0)
    col = lax.broadcasted_iota(jnp.int32, (n, n), 1)
    both = jnp.concatenate([gram, (row == col).astype(F32)], axis=1)
    wide_row = lax.broadcasted_iota(jnp.int32, (n, 2 * n), 0)
    for k in range(n):
        scale = 1.0 / jnp.sqrt(both[k : k + 1, k : k + 1])
        pivot = both[k : k + 1, :] * scale
        column = both[:, k : k + 1] * scale
        both = jnp.where(
            wide_row > k, both - column * pivot, jnp.where(wide_row == k, pivot, both)
        )
    return jnp.where(col >= row, both[:, :n], 0.0), both[:, n:]


def solve_small(count, sums, metric, cells):
    col = lax.broadcasted_iota(jnp.int32, (BLOCK, WIDE), 1)
    row = lax.broadcasted_iota(jnp.int32, (BLOCK, WIDE), 0)
    sums = sums * (1.0 / cells)
    first = jnp.where(col < count, sums, 0.0)
    square = sums[:, count : count + BLOCK]
    coeff = 2.0 * first - exact(first, metric)
    seen = exact(coeff, metric)
    gram = square - 2.0 * exact(coeff, first, nt=True) + exact(seen, coeff, nt=True)
    upper, inverse = factor(gram)
    pick = jnp.where(col == row + count, 1.0, 0.0)
    combine = exact(inverse, pick - coeff)
    left = exact(inverse, first - seen)
    return coeff, upper, combine, left


def kernel(
    nx, ny,
    v_hbm, adv_hbm, rea_hbm,
    bh, bl, qf, last, coeff1, coeff2, upper1, upper2,
    vf, adv, rea, uf, acc, hacc, metric,
    own1, first1, part1, second1, done1, whole1,
    own2, first2, part2, second2, done2, whole2,
    vsem, usem, asem, hs1, hr1, hs2, hr2,
    *sems,
):
    rows, X, Y, Z = v_hbm.shape
    main = rows - BLOCK
    cells = float(X * Y * Z * nx * ny)
    gx, gy = lax.axis_index("gx"), lax.axis_index("gy")

    def load_u(p):
        x, y = p // Y, p % Y
        return pltpu.make_async_copy(
            v_hbm.at[pl.ds(main, BLOCK), x, y], uf.at[x + 1, y + 1], usem.at[p]
        )

    def load_v(p):
        x, half = p // 2, p % 2
        lanes = pl.ds(pl.multiple_of(half * LANES, LANES), LANES)
        return pltpu.make_async_copy(v_hbm.at[pl.ds(0, main), x, :, lanes], vf.at[p], vsem.at[p])

    loop(X * Y, lambda p: load_u(p).start())
    loop(2 * X, lambda p: load_v(p).start())

    fetches = (
        pltpu.make_async_copy(adv_hbm, adv, asem.at[0]),
        pltpu.make_async_copy(rea_hbm, rea, asem.at[1]),
    )
    for fetch in fetches:
        fetch.start()

    barrier = pltpu.get_barrier_semaphore()
    for d in range(1, nx):
        pl.semaphore_signal(
            barrier, inc=1, device_id=(lax.rem(gx + d, nx), gy), device_id_type=MESH
        )
    for d in range(1, ny):
        pl.semaphore_signal(
            barrier, inc=1, device_id=(gx, lax.rem(gy + d, ny)), device_id_type=MESH
        )

    acc[...] = jnp.zeros_like(acc)
    hacc[...] = jnp.zeros_like(hacc)
    metric[...] = jnp.zeros_like(metric)
    own1[...] = jnp.zeros_like(own1)
    own2[...] = jnp.zeros_like(own2)
    edge_x = jnp.zeros((1, Y, BLOCK, Z), F32)
    edge_y = jnp.zeros((X, 1, BLOCK, Z), F32)
    for field in (uf, qf):

        @pl.when(gx == 0)
        def _(field=field):
            field[0:1, 1 : Y + 1] = edge_x

        @pl.when(gx == nx - 1)
        def _(field=field):
            field[X + 1 : X + 2, 1 : Y + 1] = edge_x

        @pl.when(gy == 0)
        def _(field=field):
            field[1 : X + 1, 0:1] = edge_y

        @pl.when(gy == ny - 1)
        def _(field=field):
            field[1 : X + 1, Y + 1 : Y + 2] = edge_y

    def borders(field, ss, rs):
        xs, ys = pl.ds(1, X), pl.ds(1, Y)
        up, down = lax.rem(gx + 1, nx), lax.rem(gx + nx - 1, nx)
        right, left = lax.rem(gy + 1, ny), lax.rem(gy + ny - 1, ny)

        def make(i, src, dst, dev):
            return pltpu.make_async_remote_copy(
                src_ref=src, dst_ref=dst, send_sem=ss.at[i], recv_sem=rs.at[i],
                device_id=dev, device_id_type=MESH,
            )

        return (
            (gx < nx - 1, gx > 0, make(0, field.at[X, ys], field.at[0, ys], (up, gy))),
            (gx > 0, gx < nx - 1, make(1, field.at[1, ys], field.at[X + 1, ys], (down, gy))),
            (gy < ny - 1, gy > 0, make(2, field.at[xs, Y], field.at[xs, 0], (gx, right))),
            (gy > 0, gy < ny - 1, make(3, field.at[xs, 1], field.at[xs, Y + 1], (gx, left))),
        )

    def send(parts):
        for sends, gets, copy in parts:
            pl.when(sends)(copy.start)

    def receive(parts):
        for sends, gets, copy in parts:
            pl.when(gets)(copy.wait_recv)

    def sent(parts):
        for sends, gets, copy in parts:
            pl.when(sends)(copy.wait_send)

    loop(X * Y, lambda p: load_u(p).wait())

    def gram(x):
        load_v(2 * x).wait()
        load_v(2 * x + 1).wait()
        slabs = [vf.at[2 * x + i].reshape(main * Y, LANES) for i in range(2)]
        for y in range(Y):
            p = x * Y + y
            vh, vl = split(jnp.concatenate([slab[pl.ds(y, main, stride=Y), :] for slab in slabs], 1))
            uh, ul = split(uf[x + 1, y + 1])
            high = jnp.concatenate([vh, uh], 0)
            low = jnp.concatenate([vl, ul], 0)
            bh[p, 0:rows, :] = high
            bl[p, 0:rows, :] = low
            r = quick(jnp.concatenate([high, low], 0), high, nt=True)
            acc[0:rows, 0:rows] += r[:rows]
            acc[WIDE : WIDE + rows, 0:rows] += r[rows:]

    gram(0)
    pl.semaphore_wait(barrier, nx - 1 + ny - 1)
    border1 = borders(uf, hs1, hr1)
    send(border1)
    loop(X - 1, lambda i: gram(i + 1))

    lane = lax.broadcasted_iota(jnp.int32, (BLOCK, Z), 1)

    def image(field, height, border):
        def step(x, ys):
            total = jnp.zeros((height + BLOCK, 2 * BLOCK), F32)
            for y in ys:
                here = field[x + 1, y + 1]
                a0 = adv[0, x, y : y + 1, :]
                a1 = adv[1, x, y : y + 1, :]
                a2 = adv[2, x, y : y + 1, :]
                below = jnp.where(lane == 0, 0.0, pltpu.roll(here, 1, 1))
                above = jnp.where(lane == Z - 1, 0.0, pltpu.roll(here, Z - 1, 1))
                near = (1.0 + a0) * field[x, y + 1] + (1.0 - a0) * field[x + 2, y + 1]
                near = near + (1.0 + a1) * field[x + 1, y] + (1.0 - a1) * field[x + 1, y + 2]
                near = near + (1.0 + a2) * below + (1.0 - a2) * above
                w = (6.0 + rea[x, y : y + 1, :]) * here - near
                p = x * Y + y
                wh, wl = split(w)
                bh[p, height : height + BLOCK, :] = wh
                bl[p, height : height + BLOCK, :] = wl
                both = jnp.concatenate([wh, wl], 0)
                total = total + quick(jnp.concatenate([bh[p, 0:height, :], wh], 0), both, nt=True)
                total = total + quick(jnp.concatenate([bl[p, 0:height, :], wl], 0), both, nt=True)
            hacc[0 : height + BLOCK, 0 : 2 * BLOCK] += total

        over_inside(X, Y, step)
        receive(border)
        over_edges(X, Y, step)
        turned = hacc[...].T
        return turned[0:BLOCK] + turned[BLOCK : 2 * BLOCK]

    for fetch in fetches:
        fetch.wait()
    dots = image(uf, rows, border1)
    cross = acc[WIDE : 2 * WIDE, :]
    local = acc[0:WIDE, :] + cross + cross.T
    own1[0:main, :] = local[0:main, 0:main]
    own1[main : main + 16, :] = local[main : main + 16, 0:main]
    own1[main + 16 : main + 32, :] = local[main : main + 16, main:WIDE]
    own1[main + 32 : main + 48, :] = dots[:, 0:main]
    own1[main + 48 : main + 64, :] = dots[:, main:WIDE]
    sum_everywhere(nx, ny, own1, first1, part1, second1, done1, whole1, sems[0:6])

    metric[0:main, 0:main] = whole1[0:main, :] * (1.0 / cells)
    metric[main : main + 16, 0:main] = whole1[main : main + 16, :] * (1.0 / cells)
    metric[main : main + 16, main:WIDE] = whole1[main + 16 : main + 32, :] * (1.0 / cells)
    metric[0:main, main:WIDE] = metric[main:WIDE, 0:main].T
    sums = jnp.concatenate([whole1[main + 32 : main + 48, :], whole1[main + 48 : main + 64, :]], 1)
    coeff, upper, combine, left = solve_small(rows, sums, metric[...], cells)
    coeff1[...] = coeff
    upper1[...] = upper

    def put_one(x, y, p, q):
        qf[x + 1, y + 1] = q
        qh, ql = split(q)
        bh[p, rows : rows + BLOCK, :] = qh
        bl[p, rows : rows + BLOCK, :] = ql

    step_one = assemble(bh, bl, X, Y, combine, rows + BLOCK, put_one)
    over_edges(X, Y, step_one)
    border2 = borders(qf, hs2, hr2)
    send(border2)
    over_inside(X, Y, step_one)

    extra = jnp.concatenate(
        [jnp.zeros((16, WIDE), F32), left, jnp.zeros((LANES - 32, WIDE), F32)], 0
    )
    metric[main:WIDE, :] += extra
    metric[0:main, main:WIDE] += extra[:, 0:main].T
    r = lax.broadcasted_iota(jnp.int32, (LANES, LANES), 0)
    c = lax.broadcasted_iota(jnp.int32, (LANES, LANES), 1)
    unit = jnp.where((r == c) & (r >= 16) & (r < 32), 1.0, 0.0)
    metric[main:WIDE, main:WIDE] += extra[:, main:WIDE].T + unit

    hacc[...] = jnp.zeros_like(hacc)
    dots = image(qf, rows + BLOCK, border2)
    own2[0:16, :] = dots[:, 0:main]
    own2[16:32, :] = dots[:, main:WIDE]
    sum_everywhere(nx, ny, own2, first2, part2, second2, done2, whole2, sems[6:12])
    sums = jnp.concatenate([whole2[0:16, :], whole2[16:32, :]], 1)
    coeff, upper, combine, left = solve_small(rows + BLOCK, sums, metric[...], cells)
    coeff2[...] = coeff
    upper2[...] = upper

    last[...] = combine
    sent(border1)
    sent(border2)


def finish(
    bh, bl, qf, last, coeff1, coeff2, upper1, upper2,
    one_hbm, two_hbm, out1, out2, factor1, factor2,
    pf, sem1, sem2,
):
    _, X, Y, _ = one_hbm.shape

    def store_one(p):
        x, y = p // Y, p % Y
        return pltpu.make_async_copy(qf.at[x + 1, y + 1], one_hbm.at[:, x, y], sem1.at[p])

    def store_two(p):
        x, y = p // Y, p % Y
        return pltpu.make_async_copy(pf.at[p], two_hbm.at[:, x, y], sem2.at[p])

    loop(X * Y, lambda p: store_one(p).start())

    def put_two(x, y, p, q):
        pf[p] = q

    step_two = assemble(bh, bl, X, Y, last[...], bh.shape[1], put_two)

    def finish_slab(x):
        step_two(x, range(Y))
        loop(Y, lambda y: store_two(x * Y + y).start())

    loop(X, finish_slab)
    rows1, rows2 = out1.shape[1], out2.shape[1]
    out1[...] = coeff1[:, 0:rows1]
    out2[...] = coeff2[:, 0:rows2]
    factor1[...] = upper1[...]
    factor2[...] = upper2[...]
    loop(X * Y, lambda p: store_one(p).wait())
    loop(X * Y, lambda p: store_two(p).wait())


def body(nx, ny, krylov_basis, advection, reaction):
    rows, X, Y, Z = krylov_basis.shape
    height1 = rows - BLOCK + 64
    height2 = max(32, 8 * nx)
    dma = pltpu.SemaphoreType.DMA
    field = jax.ShapeDtypeStruct((BLOCK, X, Y, Z), F32)
    sum_scratch = []
    for height in (height1, height2):
        sum_scratch += [
            pltpu.VMEM((height, LANES), F32),
            pltpu.VMEM((nx - 1, height // nx, LANES), F32),
            pltpu.VMEM((height // nx, LANES), F32),
            pltpu.VMEM((ny, height // nx, LANES), F32),
            pltpu.VMEM((height // nx, LANES), F32),
            pltpu.VMEM((height, LANES), F32),
        ]
    sum_sems = [dma((n - 1,)) for n in (nx, nx, ny, ny, nx, nx)] * 2
    vmem = pl.BlockSpec(memory_space=pltpu.VMEM)
    hbm = pl.BlockSpec(memory_space=pl.ANY)
    parts = ((X * Y, rows + 2 * BLOCK, Z), BF16)
    limit = 28 * 1024 * 1024
    results = pl.pallas_call(
        functools.partial(kernel, nx, ny),
        out_shape=(
            pltpu.VMEM(*parts),
            pltpu.VMEM(*parts),
            pltpu.VMEM((X + 2, Y + 2, BLOCK, Z), F32),
            pltpu.VMEM((BLOCK, WIDE), F32),
            pltpu.VMEM((BLOCK, WIDE), F32),
            pltpu.VMEM((BLOCK, WIDE), F32),
            pltpu.VMEM((BLOCK, BLOCK), F32),
            pltpu.VMEM((BLOCK, BLOCK), F32),
        ),
        in_specs=[pl.BlockSpec(memory_space=pltpu.HBM)] * 3,
        out_specs=(vmem,) * 8,
        scratch_shapes=[
            pltpu.VMEM((2 * X, rows - BLOCK, Y, LANES), F32),
            pltpu.VMEM((3, X, Y, Z), F32),
            pltpu.VMEM((X, Y, Z), F32),
            pltpu.VMEM((X + 2, Y + 2, BLOCK, Z), F32),
            pltpu.VMEM((2 * WIDE, WIDE), F32),
            pltpu.VMEM((WIDE, LANES), F32),
            pltpu.VMEM((WIDE, WIDE), F32),
        ]
        + sum_scratch
        + [dma((X * Y,))] * 2
        + [dma((2,))]
        + [dma((4,))] * 4
        + sum_sems,
        compiler_params=pltpu.CompilerParams(
            collective_id=0, has_side_effects=True, vmem_limit_bytes=limit
        ),
    )(*(pltpu.with_memory_space_constraint(a, pltpu.HBM) for a in (krylov_basis, advection, reaction)))
    one, two, out1, out2, factor1, factor2 = pl.pallas_call(
        finish,
        out_shape=(
            field,
            field,
            jax.ShapeDtypeStruct((BLOCK, rows), F32),
            jax.ShapeDtypeStruct((BLOCK, rows + BLOCK), F32),
            jax.ShapeDtypeStruct((BLOCK, BLOCK), F32),
            jax.ShapeDtypeStruct((BLOCK, BLOCK), F32),
        ),
        in_specs=[vmem] * 8,
        out_specs=(hbm, hbm, vmem, vmem, vmem, vmem),
        scratch_shapes=[pltpu.VMEM((X * Y, BLOCK, Z), F32), dma((X * Y,)), dma((X * Y,))],
        compiler_params=pltpu.CompilerParams(vmem_limit_bytes=limit),
    )(*results)
    return one, two, out1.T, out2.T, factor1, factor2


def solution(mesh):
    return jax.shard_map(
        functools.partial(body, mesh.shape["gx"], mesh.shape["gy"]),
        mesh=mesh,
        in_specs=(P(None, "gx", "gy", None), P(None, "gx", "gy", None), P("gx", "gy", None)),
        out_specs=(P(None, "gx", "gy", None), P(None, "gx", "gy", None), P(), P(), P(), P()),
        check_vma=False,
    )
```

```python
import functools

import jax
import jax.numpy as jnp
from jax import lax
from jax.experimental import pallas as pl
from jax.experimental.pallas import tpu as pltpu
from jax.sharding import PartitionSpec as P

BLOCK = 16
LANES = 128
WIDE = 256
MESH = pl.DeviceIdType.MESH
HIGHEST = lax.Precision.HIGHEST
F32 = jnp.float32
BF16 = jnp.bfloat16


def exact(left, right, nt=False):
    dims = (((1,), (1 if nt else 0,)), ((), ()))
    return lax.dot_general(left, right, dims, precision=HIGHEST, preferred_element_type=F32)


def quick(left, right, nt=False):
    dims = (((1,), (1 if nt else 0,)), ((), ()))
    return lax.dot_general(left, right, dims, preferred_element_type=F32)


def split(values):
    high = values.astype(BF16)
    low = (values - high.astype(F32)).astype(BF16)
    return high, low


def loop(n, f):
    lax.fori_loop(0, n, lambda i, c: (f(i), c)[1], 0)


def over_edges(X, Y, step):
    loop(2, lambda i: step(i * (X - 1), range(Y)))
    loop(X - 2, lambda i: step(i + 1, (0, Y - 1)))


def over_inside(X, Y, step):
    loop(X - 2, lambda i: step(i + 1, range(1, Y - 1)))


def assemble(bh, bl, X, Y, combine, height, put):
    ch, cl = split(combine)
    both = jnp.concatenate([ch, cl], 0)[:, 0:height]

    def step(x, ys):
        for y in ys:
            p = x * Y + y
            r = quick(both, bh[p, 0:height, :]) + quick(both, bl[p, 0:height, :])
            put(x, y, p, r[0:BLOCK] + r[BLOCK : 2 * BLOCK])

    return step


def sum_everywhere(nx, ny, own, first, part, second, done, whole, sems):
    gx, gy = lax.axis_index("gx"), lax.axis_index("gy")
    height = part.shape[0]
    send1, recv1, send2, recv2, send3, recv3 = sems
    mine = pl.ds(pl.multiple_of(gx * height, 8), height)
    copies = []
    for d in range(1, nx):
        peer = lax.rem(gx + d, nx)
        copies.append(
            pltpu.make_async_remote_copy(
                src_ref=own.at[pl.ds(pl.multiple_of(peer * height, 8), height)],
                dst_ref=first.at[d - 1],
                send_sem=send1.at[d - 1],
                recv_sem=recv1.at[d - 1],
                device_id=(peer, gy),
                device_id_type=MESH,
            )
        )
    for copy in copies:
        copy.start()
    yield
    for copy in copies:
        copy.wait_recv()
    total = own[mine, :]
    for d in range(1, nx):
        total = total + first[d - 1]
    part[...] = total
    second[gy] = total
    across = []
    for d in range(1, ny):
        peer = lax.rem(gy + d, ny)
        across.append(
            pltpu.make_async_remote_copy(
                src_ref=part,
                dst_ref=second.at[gy],
                send_sem=send2.at[d - 1],
                recv_sem=recv2.at[d - 1],
                device_id=(gx, peer),
                device_id_type=MESH,
            )
        )
    for copy in across:
        copy.start()
    yield
    for copy in across:
        copy.wait_recv()
    total = second[0]
    for s in range(1, ny):
        total = total + second[s]
    done[...] = total
    whole[mine, :] = total
    back = []
    for d in range(1, nx):
        peer = lax.rem(gx + d, nx)
        back.append(
            pltpu.make_async_remote_copy(
                src_ref=done,
                dst_ref=whole.at[mine],
                send_sem=send3.at[d - 1],
                recv_sem=recv3.at[d - 1],
                device_id=(peer, gy),
                device_id_type=MESH,
            )
        )
    for copy in back:
        copy.start()
    yield
    for copy in back:
        copy.wait_recv()
    for copy in copies + across + back:
        copy.wait_send()
    yield


def factor(gram):
    n = gram.shape[0]
    row = lax.broadcasted_iota(jnp.int32, (n, n), 0)
    col = lax.broadcasted_iota(jnp.int32, (n, n), 1)
    both = jnp.concatenate([gram, (row == col).astype(F32)], axis=1)
    wide_row = lax.broadcasted_iota(jnp.int32, (n, 2 * n), 0)
    for k in range(n):
        scale = 1.0 / jnp.sqrt(both[k : k + 1, k : k + 1])
        pivot = both[k : k + 1, :] * scale
        column = both[:, k : k + 1] * scale
        both = jnp.where(
            wide_row > k, both - column * pivot, jnp.where(wide_row == k, pivot, both)
        )
    return jnp.where(col >= row, both[:, :n], 0.0), both[:, n:]


def solve_small(count, sums, metric, cells):
    col = lax.broadcasted_iota(jnp.int32, (BLOCK, WIDE), 1)
    row = lax.broadcasted_iota(jnp.int32, (BLOCK, WIDE), 0)
    sums = sums * (1.0 / cells)
    first = jnp.where(col < count, sums, 0.0)
    square = sums[:, count : count + BLOCK]
    coeff = 2.0 * first - exact(first, metric)
    seen = exact(coeff, metric)
    gram = square - 2.0 * exact(coeff, first, nt=True) + exact(seen, coeff, nt=True)
    upper, inverse = factor(gram)
    pick = jnp.where(col == row + count, 1.0, 0.0)
    combine = exact(inverse, pick - coeff)
    left = exact(inverse, first - seen)
    return coeff, upper, combine, left


def kernel(
    nx, ny,
    v_hbm, adv_hbm, rea_hbm,
    bh, bl, qf, last, coeff1, coeff2, upper1, upper2,
    vf, adv, rea, uf, acc, hacc, metric,
    own1, first1, part1, second1, done1, whole1,
    own2, first2, part2, second2, done2, whole2,
    own3, first3, part3, second3, done3, whole3,
    vsem, usem, asem, hs1, hr1, hs2, hr2,
    *sems,
):
    rows, X, Y, Z = v_hbm.shape
    main = rows - BLOCK
    cells = float(X * Y * Z * nx * ny)
    gx, gy = lax.axis_index("gx"), lax.axis_index("gy")

    def load_u(p):
        x, y = p // Y, p % Y
        return pltpu.make_async_copy(
            v_hbm.at[pl.ds(main, BLOCK), x, y], uf.at[x + 1, y + 1], usem.at[p]
        )

    def load_v(p):
        x, half = p // 2, p % 2
        lanes = pl.ds(pl.multiple_of(half * LANES, LANES), LANES)
        return pltpu.make_async_copy(v_hbm.at[pl.ds(0, main), x, :, lanes], vf.at[p], vsem.at[p])

    loop(X * Y, lambda p: load_u(p).start())
    loop(2 * X, lambda p: load_v(p).start())

    fetches = (
        pltpu.make_async_copy(adv_hbm, adv, asem.at[0]),
        pltpu.make_async_copy(rea_hbm, rea, asem.at[1]),
    )
    for fetch in fetches:
        fetch.start()

    barrier = pltpu.get_barrier_semaphore()
    for d in range(1, nx):
        pl.semaphore_signal(
            barrier, inc=1, device_id=(lax.rem(gx + d, nx), gy), device_id_type=MESH
        )
    for d in range(1, ny):
        pl.semaphore_signal(
            barrier, inc=1, device_id=(gx, lax.rem(gy + d, ny)), device_id_type=MESH
        )

    acc[...] = jnp.zeros_like(acc)
    hacc[...] = jnp.zeros_like(hacc)
    metric[...] = jnp.zeros_like(metric)
    own1[...] = jnp.zeros_like(own1)
    own2[...] = jnp.zeros_like(own2)
    own3[...] = jnp.zeros_like(own3)
    edge_x = jnp.zeros((1, Y, BLOCK, Z), F32)
    edge_y = jnp.zeros((X, 1, BLOCK, Z), F32)
    for field in (uf, qf):

        @pl.when(gx == 0)
        def _(field=field):
            field[0:1, 1 : Y + 1] = edge_x

        @pl.when(gx == nx - 1)
        def _(field=field):
            field[X + 1 : X + 2, 1 : Y + 1] = edge_x

        @pl.when(gy == 0)
        def _(field=field):
            field[1 : X + 1, 0:1] = edge_y

        @pl.when(gy == ny - 1)
        def _(field=field):
            field[1 : X + 1, Y + 1 : Y + 2] = edge_y

    def borders(field, ss, rs):
        xs, ys = pl.ds(1, X), pl.ds(1, Y)
        up, down = lax.rem(gx + 1, nx), lax.rem(gx + nx - 1, nx)
        right, left = lax.rem(gy + 1, ny), lax.rem(gy + ny - 1, ny)

        def make(i, src, dst, dev):
            return pltpu.make_async_remote_copy(
                src_ref=src, dst_ref=dst, send_sem=ss.at[i], recv_sem=rs.at[i],
                device_id=dev, device_id_type=MESH,
            )

        return (
            (gx < nx - 1, gx > 0, make(0, field.at[X, ys], field.at[0, ys], (up, gy))),
            (gx > 0, gx < nx - 1, make(1, field.at[1, ys], field.at[X + 1, ys], (down, gy))),
            (gy < ny - 1, gy > 0, make(2, field.at[xs, Y], field.at[xs, 0], (gx, right))),
            (gy > 0, gy < ny - 1, make(3, field.at[xs, 1], field.at[xs, Y + 1], (gx, left))),
        )

    def send(parts):
        for sends, gets, copy in parts:
            pl.when(sends)(copy.start)

    def receive(parts):
        for sends, gets, copy in parts:
            pl.when(gets)(copy.wait_recv)

    def sent(parts):
        for sends, gets, copy in parts:
            pl.when(sends)(copy.wait_send)

    loop(X * Y, lambda p: load_u(p).wait())

    def gram(x):
        load_v(2 * x).wait()
        load_v(2 * x + 1).wait()
        slabs = [vf.at[2 * x + i].reshape(main * Y, LANES) for i in range(2)]
        for y in range(Y):
            p = x * Y + y
            vh, vl = split(jnp.concatenate([slab[pl.ds(y, main, stride=Y), :] for slab in slabs], 1))
            uh, ul = split(uf[x + 1, y + 1])
            high = jnp.concatenate([vh, uh], 0)
            low = jnp.concatenate([vl, ul], 0)
            bh[p, 0:rows, :] = high
            bl[p, 0:rows, :] = low
            r = quick(jnp.concatenate([high, low], 0), high, nt=True)
            acc[0:rows, 0:rows] += r[:rows]
            acc[WIDE : WIDE + rows, 0:rows] += r[rows:]

    gram(0)
    pl.semaphore_wait(barrier, nx - 1 + ny - 1)
    border1 = borders(uf, hs1, hr1)
    send(border1)
    loop(X - 1, lambda i: gram(i + 1))

    lane = lax.broadcasted_iota(jnp.int32, (BLOCK, Z), 1)

    def image(field, height, border, between=None):
        def step(x, ys):
            total = jnp.zeros((height + BLOCK, 2 * BLOCK), F32)
            for y in ys:
                here = field[x + 1, y + 1]
                a0 = adv[0, x, y : y + 1, :]
                a1 = adv[1, x, y : y + 1, :]
                a2 = adv[2, x, y : y + 1, :]
                below = jnp.where(lane == 0, 0.0, pltpu.roll(here, 1, 1))
                above = jnp.where(lane == Z - 1, 0.0, pltpu.roll(here, Z - 1, 1))
                near = (1.0 + a0) * field[x, y + 1] + (1.0 - a0) * field[x + 2, y + 1]
                near = near + (1.0 + a1) * field[x + 1, y] + (1.0 - a1) * field[x + 1, y + 2]
                near = near + (1.0 + a2) * below + (1.0 - a2) * above
                w = (6.0 + rea[x, y : y + 1, :]) * here - near
                p = x * Y + y
                wh, wl = split(w)
                bh[p, height : height + BLOCK, :] = wh
                bl[p, height : height + BLOCK, :] = wl
                both = jnp.concatenate([wh, wl], 0)
                total = total + quick(jnp.concatenate([bh[p, 0:height, :], wh], 0), both, nt=True)
                total = total + quick(jnp.concatenate([bl[p, 0:height, :], wl], 0), both, nt=True)
            hacc[0 : height + BLOCK, 0 : 2 * BLOCK] += total

        over_inside(X, Y, step)
        receive(border)
        if between is not None:
            next(between)
        over_edges(X, Y, step)
        turned = hacc[...].T
        return turned[0:BLOCK] + turned[BLOCK : 2 * BLOCK]

    for fetch in fetches:
        fetch.wait()
    cross = acc[WIDE : 2 * WIDE, :]
    local = acc[0:WIDE, :] + cross + cross.T
    own1[0:main, :] = local[0:main, 0:main]
    own1[main : main + 16, :] = local[main : main + 16, 0:main]
    own1[main + 16 : main + 32, :] = local[main : main + 16, main:WIDE]
    bases_sum = sum_everywhere(nx, ny, own1, first1, part1, second1, done1, whole1, sems[0:6])
    next(bases_sum)
    dots = image(uf, rows, border1, bases_sum)
    own2[0:16, :] = dots[:, 0:main]
    own2[16:32, :] = dots[:, main:WIDE]
    image_sum = sum_everywhere(nx, ny, own2, first2, part2, second2, done2, whole2, sems[6:12])
    next(image_sum)
    next(bases_sum)
    next(image_sum)
    next(bases_sum)
    next(image_sum)
    next(image_sum)

    metric[0:main, 0:main] = whole1[0:main, :] * (1.0 / cells)
    metric[main : main + 16, 0:main] = whole1[main : main + 16, :] * (1.0 / cells)
    metric[main : main + 16, main:WIDE] = whole1[main + 16 : main + 32, :] * (1.0 / cells)
    metric[0:main, main:WIDE] = metric[main:WIDE, 0:main].T
    sums = jnp.concatenate([whole2[0:16, :], whole2[16:32, :]], 1)
    coeff, upper, combine, left = solve_small(rows, sums, metric[...], cells)
    coeff1[...] = coeff
    upper1[...] = upper

    def put_one(x, y, p, q):
        qf[x + 1, y + 1] = q
        qh, ql = split(q)
        bh[p, rows : rows + BLOCK, :] = qh
        bl[p, rows : rows + BLOCK, :] = ql

    step_one = assemble(bh, bl, X, Y, combine, rows + BLOCK, put_one)
    over_edges(X, Y, step_one)
    border2 = borders(qf, hs2, hr2)
    send(border2)
    over_inside(X, Y, step_one)

    extra = jnp.concatenate(
        [jnp.zeros((16, WIDE), F32), left, jnp.zeros((LANES - 32, WIDE), F32)], 0
    )
    metric[main:WIDE, :] += extra
    metric[0:main, main:WIDE] += extra[:, 0:main].T
    r = lax.broadcasted_iota(jnp.int32, (LANES, LANES), 0)
    c = lax.broadcasted_iota(jnp.int32, (LANES, LANES), 1)
    unit = jnp.where((r == c) & (r >= 16) & (r < 32), 1.0, 0.0)
    metric[main:WIDE, main:WIDE] += extra[:, main:WIDE].T + unit

    hacc[...] = jnp.zeros_like(hacc)
    dots = image(qf, rows + BLOCK, border2)
    own3[0:16, :] = dots[:, 0:main]
    own3[16:32, :] = dots[:, main:WIDE]
    for _ in sum_everywhere(nx, ny, own3, first3, part3, second3, done3, whole3, sems[12:18]):
        pass
    sums = jnp.concatenate([whole3[0:16, :], whole3[16:32, :]], 1)
    coeff, upper, combine, left = solve_small(rows + BLOCK, sums, metric[...], cells)
    coeff2[...] = coeff
    upper2[...] = upper

    last[...] = combine
    sent(border1)
    sent(border2)


def finish(
    bh, bl, qf, last, coeff1, coeff2, upper1, upper2,
    one_hbm, two_hbm, out1, out2, factor1, factor2,
    pf, sem1, sem2,
):
    _, X, Y, _ = one_hbm.shape

    def store_one(p):
        x, y = p // Y, p % Y
        return pltpu.make_async_copy(qf.at[x + 1, y + 1], one_hbm.at[:, x, y], sem1.at[p])

    def store_two(p):
        x, y = p // Y, p % Y
        return pltpu.make_async_copy(pf.at[p], two_hbm.at[:, x, y], sem2.at[p])

    loop(X * Y, lambda p: store_one(p).start())

    def put_two(x, y, p, q):
        pf[p] = q

    step_two = assemble(bh, bl, X, Y, last[...], bh.shape[1], put_two)

    def finish_slab(x):
        step_two(x, range(Y))
        loop(Y, lambda y: store_two(x * Y + y).start())

    loop(X, finish_slab)
    rows1, rows2 = out1.shape[1], out2.shape[1]
    out1[...] = coeff1[:, 0:rows1]
    out2[...] = coeff2[:, 0:rows2]
    factor1[...] = upper1[...]
    factor2[...] = upper2[...]
    loop(X * Y, lambda p: store_one(p).wait())
    loop(X * Y, lambda p: store_two(p).wait())


def body(nx, ny, krylov_basis, advection, reaction):
    rows, X, Y, Z = krylov_basis.shape
    height1 = -(-(rows + BLOCK) // (8 * nx)) * (8 * nx)
    height2 = max(32, 8 * nx)
    dma = pltpu.SemaphoreType.DMA
    field = jax.ShapeDtypeStruct((BLOCK, X, Y, Z), F32)
    sum_scratch = []
    for height in (height1, height2, height2):
        sum_scratch += [
            pltpu.VMEM((height, LANES), F32),
            pltpu.VMEM((nx - 1, height // nx, LANES), F32),
            pltpu.VMEM((height // nx, LANES), F32),
            pltpu.VMEM((ny, height // nx, LANES), F32),
            pltpu.VMEM((height // nx, LANES), F32),
            pltpu.VMEM((height, LANES), F32),
        ]
    sum_sems = [dma((n - 1,)) for n in (nx, nx, ny, ny, nx, nx)] * 3
    vmem = pl.BlockSpec(memory_space=pltpu.VMEM)
    hbm = pl.BlockSpec(memory_space=pl.ANY)
    parts = ((X * Y, rows + 2 * BLOCK, Z), BF16)
    limit = 28 * 1024 * 1024
    results = pl.pallas_call(
        functools.partial(kernel, nx, ny),
        out_shape=(
            pltpu.VMEM(*parts),
            pltpu.VMEM(*parts),
            pltpu.VMEM((X + 2, Y + 2, BLOCK, Z), F32),
            pltpu.VMEM((BLOCK, WIDE), F32),
            pltpu.VMEM((BLOCK, WIDE), F32),
            pltpu.VMEM((BLOCK, WIDE), F32),
            pltpu.VMEM((BLOCK, BLOCK), F32),
            pltpu.VMEM((BLOCK, BLOCK), F32),
        ),
        in_specs=[pl.BlockSpec(memory_space=pltpu.HBM)] * 3,
        out_specs=(vmem,) * 8,
        scratch_shapes=[
            pltpu.VMEM((2 * X, rows - BLOCK, Y, LANES), F32),
            pltpu.VMEM((3, X, Y, Z), F32),
            pltpu.VMEM((X, Y, Z), F32),
            pltpu.VMEM((X + 2, Y + 2, BLOCK, Z), F32),
            pltpu.VMEM((2 * WIDE, WIDE), F32),
            pltpu.VMEM((WIDE, LANES), F32),
            pltpu.VMEM((WIDE, WIDE), F32),
        ]
        + sum_scratch
        + [dma((X * Y,))] * 2
        + [dma((2,))]
        + [dma((4,))] * 4
        + sum_sems,
        compiler_params=pltpu.CompilerParams(
            collective_id=0, has_side_effects=True, vmem_limit_bytes=limit
        ),
    )(*(pltpu.with_memory_space_constraint(a, pltpu.HBM) for a in (krylov_basis, advection, reaction)))
    one, two, out1, out2, factor1, factor2 = pl.pallas_call(
        finish,
        out_shape=(
            field,
            field,
            jax.ShapeDtypeStruct((BLOCK, rows), F32),
            jax.ShapeDtypeStruct((BLOCK, rows + BLOCK), F32),
            jax.ShapeDtypeStruct((BLOCK, BLOCK), F32),
            jax.ShapeDtypeStruct((BLOCK, BLOCK), F32),
        ),
        in_specs=[vmem] * 8,
        out_specs=(hbm, hbm, vmem, vmem, vmem, vmem),
        scratch_shapes=[pltpu.VMEM((X * Y, BLOCK, Z), F32), dma((X * Y,)), dma((X * Y,))],
        compiler_params=pltpu.CompilerParams(vmem_limit_bytes=limit),
    )(*results)
    return one, two, out1.T, out2.T, factor1, factor2


def solution(mesh):
    return jax.shard_map(
        functools.partial(body, mesh.shape["gx"], mesh.shape["gy"]),
        mesh=mesh,
        in_specs=(P(None, "gx", "gy", None), P(None, "gx", "gy", None), P("gx", "gy", None)),
        out_specs=(P(None, "gx", "gy", None), P(None, "gx", "gy", None), P(), P(), P(), P()),
        check_vma=False,
    )
```
